32 devices in a mesh: task: 4 (over y, core), param: 8 (over z, x).
Axes of the slice: x: 2, y: 2, z: 4, core: 2. Of those that a mesh axis runs over, the one named last changes fastest.
Arguments:
- params: bfloat16 [16, 512, 4096], P('task', 'param'), may hold values from -6 to 6
- fisher: float32 [16, 512, 4096], P('task', 'param'), may hold values from 3e-06 to 1, as said below
Outputs:
- merged: bfloat16 [512, 4096], P('param')
The draws below stay inside these ranges and needn't reach their ends.
Inputs may be any that keep to these rules, and one draw needn't show every extreme that they name: `fisher`: every entry is positive; scales differ strongly between tasks and between regions of rows.
All inputs are finite; a program needn't handle non-finite values.
Results may differ from the reference program's by a relative error of at most 0.00045.
Values may be sent and summed in bfloat16 or wider, within the bound.
A program may use at most 64 MiB of HBM per device.

```python
import math
import jax
import jax.numpy as jnp
from jax import lax

FF = 4096
TASKS = 16
ROWS = 512


def draw_fisher(key, part):
    first, second, third = jax.random.split(key, 3)
    region = jnp.exp(jax.random.uniform(first, (TASKS, 8), jnp.float32, math.log(1.0 / 256.0), 0.0))
    region = jnp.repeat(region, ROWS // 8, axis=1)
    base = jnp.exp(jax.random.uniform(second, (TASKS, ROWS, FF), jnp.float32, math.log(0.001), 0.0))
    return (base * region[:, :, None]).astype(jnp.float32)


def block_levels(own_key, dims, cuts, least, top_value):
    gain, own = 1.0, jax.random.fold_in(own_key, 6)
    for position, blocks in cuts:
        draws = jnp.exp(jax.random.uniform(jax.random.fold_in(own, position), (blocks,), jnp.float32, least / len(cuts), top_value / len(cuts)))
        gain = gain * jnp.repeat(draws, dims[position] // blocks).reshape([-1 if axis == position else 1 for axis in range(len(dims))])
    return gain


def scatter_about(own_key, dims, spread, bound, shards=(), kind=jnp.bfloat16):
    factor_of = block_levels(own_key, dims, shards, -0.22, 0.18) if shards else 1.0
    values = jax.random.normal(own_key, dims, jnp.float32) * spread * factor_of
    return jnp.minimum(jnp.maximum(values, -bound), bound).astype(kind)


def setup_inputs(seed: int = 0) -> dict:
    arg_keys = jax.random.split(jax.random.key(seed), 3)
    return {
        "params": scatter_about(arg_keys[0], (TASKS, ROWS, FF), 1.0, 6.0, ((0, 4), (1, 8))),
        "fisher": draw_fisher(jax.random.fold_in(arg_keys[2], 71), 0),
    }


def reference(params, fisher):
    peak = jnp.max(fisher, axis=(1, 2))
    total = jnp.sum(fisher, axis=(1, 2))
    count = float(ROWS * FF)
    factor = count * peak / total

    def one_task(carry, items):
        theta, info, top, mult = items
        weight = jnp.clip(info / top, 0.002, 0.25) * mult
        return (carry[0] + weight * theta.astype(jnp.float32), carry[1] + weight), None

    start = (jnp.zeros((ROWS, FF), jnp.float32), jnp.zeros((ROWS, FF), jnp.float32))
    sums, unused = lax.scan(one_task, start, (params, fisher, peak, factor))
    return (sums[0] / sums[1]).astype(jnp.bfloat16)
```

```python
import functools

import jax
import jax.numpy as jnp
from jax import lax
from jax.experimental import pallas as pl
from jax.experimental.pallas import tpu as pltpu
from jax.sharding import PartitionSpec as P

MESH = pl.DeviceIdType.MESH
LANES = 128
PIECES = 8


def kernel(tasks, groups, params_hbm, fisher_hbm, out, fisher, params, stats, give, take, bound, kept, landed,
           load_f, load_p, stat_send, stat_recv, give_send, give_recv, y_send, y_recv, res_send, res_recv,
           near_send, near_recv):
    count, rows, width = fisher.shape
    chips = tasks // 2
    chunks, chunk = give.shape[2], give.shape[5]
    half, piece = width // 2, width // tasks
    task, param = lax.axis_index("task"), lax.axis_index("param")
    chip, core = task // 2, task % 2
    partner = {"task": chip * 2 + 1 - core, "param": param}

    def chip_at(shift):
        return lax.rem(chip + shift, chips)

    def same_core(shift):
        return {"task": chip_at(shift) * 2 + core, "param": param}

    def member(shift):
        return {"task": task, "param": lax.rem(param + shift, groups)}

    loads_f = [pltpu.make_async_copy(fisher_hbm.at[t], fisher.at[t], load_f.at[t]) for t in range(count)]
    loads_p = [pltpu.make_async_copy(params_hbm.at[t], params.at[t], load_p.at[t]) for t in range(count)]
    for copy in loads_f + loads_p:
        copy.start()

    barrier = pltpu.get_barrier_semaphore()
    greeted = [member(s) for s in range(1, groups)] + [partner] + [same_core(s) for s in range(1, chips)]
    for device in greeted:
        pl.semaphore_signal(barrier, inc=1, device_id=device, device_id_type=MESH)

    tops, sums = [], []
    for t in range(count):
        loads_f[t].wait()

        def over(step, carry, t=t):
            block = fisher[t, :, pl.ds(pl.multiple_of(step * LANES, LANES), LANES)]
            return jnp.maximum(carry[0], block), carry[1] + block

        first = fisher[t, :, 0:LANES]
        top, total = lax.fori_loop(1, width // LANES, over, (first, first), unroll=8)
        tops.append(jnp.max(top, axis=0, keepdims=True))
        sums.append(jnp.sum(total, axis=0, keepdims=True))
    top = jnp.max(jnp.concatenate(tops, axis=0), axis=1, keepdims=True)
    total = jnp.sum(jnp.concatenate(sums, axis=0), axis=1, keepdims=True)
    stats[0, 0:count, :] = jnp.broadcast_to(top, (count, LANES))
    stats[0, count:2 * count, :] = jnp.broadcast_to(total, (count, LANES))

    pl.semaphore_wait(barrier, len(greeted))

    stat_copies = [
        pltpu.make_async_remote_copy(
            src_ref=stats.at[0], dst_ref=stats.at[s], send_sem=stat_send.at[s], recv_sem=stat_recv.at[s],
            device_id=member(s), device_id_type=MESH)
        for s in range(1, groups)
    ]
    for copy in stat_copies:
        copy.start()
    for copy in loads_p:
        copy.wait()
    for copy in stat_copies:
        copy.wait_recv()
    peak, total = stats[0, 0:count, :], stats[0, count:2 * count, :]
    for s in range(1, groups):
        peak = jnp.maximum(peak, stats[s, 0:count, :])
        total = total + stats[s, count:2 * count, :]
    size = float(rows * groups * width)
    gain = size / total
    factor = peak * gain
    low, high = 0.002 * factor, 0.25 * factor
    spread = [
        tuple(jnp.broadcast_to(a[t:t + 1, :], (rows, LANES)) for a in (gain, low, high)) for t in range(count)
    ]

    def partial(side, target, k):
        numers, denoms = [], []
        for part in range(chunk // LANES):
            start = pl.multiple_of(side * half + target * piece + k * chunk + part * LANES, LANES)
            numer = denom = None
            for t in range(count):
                gain_t, low_t, high_t = spread[t]
                info = fisher[t, :, pl.ds(start, LANES)]
                theta = params[t, :, pl.ds(start, LANES)].astype(jnp.float32)
                weight = jnp.minimum(jnp.maximum(info * gain_t, low_t), high_t)
                numer = weight * theta if t == 0 else numer + weight * theta
                denom = weight if t == 0 else denom + weight
            numers.append(numer)
            denoms.append(denom)
        if len(numers) == 1:
            return numers[0], denoms[0]
        return jnp.concatenate(numers, axis=1), jnp.concatenate(denoms, axis=1)

    def put(ref, pair):
        ref[0], ref[1] = pair

    def added(one, two):
        return one[0] + two[0], one[1] + two[1]

    def give_copy(shift, k):
        return pltpu.make_async_remote_copy(
            src_ref=give.at[shift, 0, k], dst_ref=take.at[shift, 0, k], send_sem=give_send.at[shift, k],
            recv_sem=give_recv.at[shift, k], device_id=partner, device_id_type=MESH)

    def y_copy(shift, k):
        return pltpu.make_async_remote_copy(
            src_ref=bound.at[shift - 1, k], dst_ref=landed.at[shift - 1, k], send_sem=y_send.at[shift - 1, k],
            recv_sem=y_recv.at[shift - 1, k], device_id=same_core(shift), device_id_type=MESH)

    def columns(side, target, k):
        return pl.ds(pl.multiple_of(side * half + target * piece + k * chunk, LANES), chunk)

    def res_copy(shift, k):
        where = out.at[:, columns(core, chip, k)]
        return pltpu.make_async_remote_copy(
            src_ref=where, dst_ref=where, send_sem=res_send.at[shift - 1, k], recv_sem=res_recv.at[shift - 1, k],
            device_id=same_core(shift), device_id_type=MESH)

    def near_copy(shift, k):
        where = out.at[:, columns(core, chip_at(chips - shift), k)]
        return pltpu.make_async_remote_copy(
            src_ref=where, dst_ref=where, send_sem=near_send.at[shift, k], recv_sem=near_recv.at[shift, k],
            device_id=partner, device_id_type=MESH)

    away = [(shift, k) for k in range(chunks) for shift in range(1, chips)]
    gives = {}

    def hand_over(shift, k):
        put(give.at[shift, 0, k], partial(1 - core, chip_at(shift), k))
        gives[shift, k] = give_copy(shift, k)
        gives[shift, k].start()

    for shift, k in away:
        hand_over(shift, k)
    for shift, k in away:
        put(bound.at[shift - 1, k], partial(core, chip_at(shift), k))
    y_copies = {}
    for shift, k in away:
        gives[shift, k].wait_recv()
        put(bound.at[shift - 1, k], added(bound.at[shift - 1, k], take.at[shift, 0, k]))
        y_copies[shift, k] = y_copy(shift, k)
        y_copies[shift, k].start()
    for k in range(chunks):
        hand_over(0, k)
    for k in range(chunks):
        put(kept.at[k], partial(core, chip, k))
    for k in range(chunks):
        gives[0, k].wait_recv()
        put(kept.at[k], added(kept.at[k], take.at[0, 0, k]))

    res_copies, near_copies = {}, {}
    for k in range(chunks):
        total = kept[k, 0], kept[k, 1]
        for shift in range(1, chips):
            y_copies[shift, k].wait_recv()
            total = added(total, landed.at[shift - 1, k])
        out[:, columns(core, chip, k)] = (total[0] / total[1]).astype(out.dtype)
        for shift in range(1, chips):
            res_copies[shift, k] = res_copy(shift, k)
            res_copies[shift, k].start()
        near_copies[0, k] = near_copy(0, k)
        near_copies[0, k].start()
    for shift, k in away:
        res_copies[shift, k].wait_recv()
        near_copies[shift, k] = near_copy(shift, k)
        near_copies[shift, k].start()
    for copies in (gives, y_copies, res_copies):
        for copy in copies.values():
            copy.wait_send()
    for copy in stat_copies:
        copy.wait_send()
    for copy in near_copies.values():
        copy.wait()


def local(mesh, params, fisher):
    count, rows, width = fisher.shape
    tasks, groups = mesh.shape["task"], mesh.shape["param"]
    chips, piece = tasks // 2, width // tasks
    chunks = max(1, min(PIECES, piece // LANES))
    chunk = piece // chunks
    far = max(1, chips - 1)
    f32, dma = jnp.float32, pltpu.SemaphoreType.DMA
    return pl.pallas_call(
        functools.partial(kernel, tasks, groups),
        out_shape=pltpu.VMEM((rows, width), jnp.bfloat16),
        in_specs=[pl.BlockSpec(memory_space=pltpu.HBM)] * 2,
        out_specs=pl.BlockSpec(memory_space=pltpu.VMEM),
        scratch_shapes=[
            pltpu.VMEM((count, rows, width), f32),
            pltpu.VMEM((count, rows, width), jnp.bfloat16),
            pltpu.VMEM((groups, 2 * count, LANES), f32),
            pltpu.VMEM((chips, 1, chunks, 2, rows, chunk), f32),
            pltpu.VMEM((chips, 1, chunks, 2, rows, chunk), f32),
            pltpu.VMEM((far, chunks, 2, rows, chunk), f32),
            pltpu.VMEM((chunks, 2, rows, chunk), f32),
            pltpu.VMEM((far, chunks, 2, rows, chunk), f32),
            dma((count,)),
            dma((count,)),
            dma((groups,)),
            dma((groups,)),
            dma((chips, chunks)),
            dma((chips, chunks)),
            dma((far, chunks)),
            dma((far, chunks)),
            dma((far, chunks)),
            dma((far, chunks)),
            dma((chips, chunks)),
            dma((chips, chunks)),
        ],
        compiler_params=pltpu.CompilerParams(collective_id=0, has_side_effects=True),
        name="merge",
    )(params, fisher)


def solution(mesh):
    in_specs = (P("task", "param", None), P("task", "param", None))
    out_specs = P("param", None)
    return jax.shard_map(
        functools.partial(local, mesh), mesh=mesh, in_specs=in_specs, out_specs=out_specs, check_vma=False)
```

```python
import functools

import jax
import jax.numpy as jnp
from jax import lax
from jax.experimental import pallas as pl
from jax.experimental.pallas import tpu as pltpu
from jax.sharding import PartitionSpec as P

MESH = pl.DeviceIdType.MESH
LANES = 128
PIECES = 8


def split(value):
    scaled = value * 257.0
    kept = scaled - (scaled - value)
    low = kept * 0.74
    scaled = low * 8388609.0
    return kept, scaled - (scaled - low)


def coded(numer, denom):
    top = numer.astype(jnp.bfloat16)
    wide = top.astype(jnp.float32)
    rest = (numer - wide) / jnp.where(wide == 0.0, 1.0, wide)
    rest = jnp.clip(jnp.round(rest * 32768.0), -127.0, 127.0)
    kept, power = split(denom)
    return kept + rest * (power * (1.0 / 8388608.0)), top


def decoded(carrier, top):
    kept, power = split(carrier)
    wide = top.astype(jnp.float32)
    return wide + wide * ((carrier - kept) / power * 256.0), kept


def kernel(tasks, groups, params_hbm, fisher_hbm, out, fisher, params, stats, give, take, bound, kept,
           wide_out, top_out, wide_in, top_in,
           load_f, load_p, stat_send, stat_recv, give_send, give_recv, y_send, y_recv, top_send, top_recv,
           res_send, res_recv, near_send, near_recv):
    count, rows, width = fisher.shape
    chips = tasks // 2
    chunks, chunk = give.shape[2], give.shape[5]
    half, piece = width // 2, width // tasks
    task, param = lax.axis_index("task"), lax.axis_index("param")
    chip, core = task // 2, task % 2
    partner = {"task": chip * 2 + 1 - core, "param": param}

    def chip_at(shift):
        return lax.rem(chip + shift, chips)

    def same_core(shift):
        return {"task": chip_at(shift) * 2 + core, "param": param}

    def member(shift):
        return {"task": task, "param": lax.rem(param + shift, groups)}

    loads_f = [pltpu.make_async_copy(fisher_hbm.at[t], fisher.at[t], load_f.at[t]) for t in range(count)]
    loads_p = [pltpu.make_async_copy(params_hbm.at[t], params.at[t], load_p.at[t]) for t in range(count)]
    for copy in loads_f:
        copy.start()

    barrier = pltpu.get_barrier_semaphore()
    greeted = [member(s) for s in range(1, groups)] + [partner] + [same_core(s) for s in range(1, chips)]
    for device in greeted:
        pl.semaphore_signal(barrier, inc=1, device_id=device, device_id_type=MESH)

    tops, sums = [], []
    for t in range(count):
        loads_f[t].wait()
        if t == count - 1:
            for copy in loads_p:
                copy.start()

        def over(step, carry, t=t):
            block = fisher[t, :, pl.ds(pl.multiple_of(step * LANES, LANES), LANES)]
            return jnp.maximum(carry[0], block), carry[1] + block

        first = fisher[t, :, 0:LANES]
        top, total = lax.fori_loop(1, width // LANES, over, (first, first), unroll=8)
        tops.append(jnp.max(top, axis=0, keepdims=True))
        sums.append(jnp.sum(total, axis=0, keepdims=True))
    top = jnp.max(jnp.concatenate(tops, axis=0), axis=1, keepdims=True)
    total = jnp.sum(jnp.concatenate(sums, axis=0), axis=1, keepdims=True)
    stats[0, 0:count, :] = jnp.broadcast_to(top, (count, LANES))
    stats[0, count:2 * count, :] = jnp.broadcast_to(total, (count, LANES))

    pl.semaphore_wait(barrier, len(greeted))

    stat_copies = [
        pltpu.make_async_remote_copy(
            src_ref=stats.at[0], dst_ref=stats.at[s], send_sem=stat_send.at[s], recv_sem=stat_recv.at[s],
            device_id=member(s), device_id_type=MESH)
        for s in range(1, groups)
    ]
    for copy in stat_copies:
        copy.start()
    for copy in loads_p:
        copy.wait()
    for copy in stat_copies:
        copy.wait_recv()
    peak, total = stats[0, 0:count, :], stats[0, count:2 * count, :]
    for s in range(1, groups):
        peak = jnp.maximum(peak, stats[s, 0:count, :])
        total = total + stats[s, count:2 * count, :]
    size = float(rows * groups * width)
    gain = size / total
    factor = peak * gain
    low, high = 0.002 * factor, 0.25 * factor
    spread = [
        tuple(jnp.broadcast_to(a[t:t + 1, :], (rows, LANES)) for a in (gain, low, high)) for t in range(count)
    ]

    def partial(side, target, k):
        numers, denoms = [], []
        for part in range(chunk // LANES):
            start = pl.multiple_of(side * half + target * piece + k * chunk + part * LANES, LANES)
            numer = denom = None
            for t in range(count):
                gain_t, low_t, high_t = spread[t]
                info = fisher[t, :, pl.ds(start, LANES)]
                theta = params[t, :, pl.ds(start, LANES)].astype(jnp.float32)
                weight = jnp.minimum(jnp.maximum(info * gain_t, low_t), high_t)
                numer = weight * theta if t == 0 else numer + weight * theta
                denom = weight if t == 0 else denom + weight
            numers.append(numer)
            denoms.append(denom)
        if len(numers) == 1:
            return numers[0], denoms[0]
        return jnp.concatenate(numers, axis=1), jnp.concatenate(denoms, axis=1)

    def put(ref, pair):
        ref[0], ref[1] = pair

    def added(one, two):
        return one[0] + two[0], one[1] + two[1]

    def give_copy(shift, k):
        return pltpu.make_async_remote_copy(
            src_ref=give.at[shift, 0, k], dst_ref=take.at[shift, 0, k], send_sem=give_send.at[shift, k],
            recv_sem=give_recv.at[shift, k], device_id=partner, device_id_type=MESH)

    def y_copy(shift, k):
        return [
            pltpu.make_async_remote_copy(
                src_ref=source.at[shift - 1, k], dst_ref=sink.at[shift - 1, k], send_sem=send.at[shift - 1, k],
                recv_sem=recv.at[shift - 1, k], device_id=same_core(shift), device_id_type=MESH)
            for source, sink, send, recv in (
                (wide_out, wide_in, y_send, y_recv), (top_out, top_in, top_send, top_recv))
        ]

    def columns(side, target, k):
        return pl.ds(pl.multiple_of(side * half + target * piece + k * chunk, LANES), chunk)

    def res_copy(shift, k):
        where = out.at[:, columns(core, chip, k)]
        return pltpu.make_async_remote_copy(
            src_ref=where, dst_ref=where, send_sem=res_send.at[shift - 1, k], recv_sem=res_recv.at[shift - 1, k],
            device_id=same_core(shift), device_id_type=MESH)

    def near_copy(shift, k):
        where = out.at[:, columns(core, chip_at(chips - shift), k)]
        return pltpu.make_async_remote_copy(
            src_ref=where, dst_ref=where, send_sem=near_send.at[shift, k], recv_sem=near_recv.at[shift, k],
            device_id=partner, device_id_type=MESH)

    away = [(shift, k) for k in range(chunks) for shift in range(1, chips)]
    gives = {}

    def hand_over(shift, k):
        put(give.at[shift, 0, k], partial(1 - core, chip_at(shift), k))
        gives[shift, k] = give_copy(shift, k)
        gives[shift, k].start()

    for shift, k in away:
        hand_over(shift, k)
    for shift, k in away:
        put(bound.at[shift - 1, k], partial(core, chip_at(shift), k))
    y_copies = {}
    for shift, k in away:
        gives[shift, k].wait_recv()
        wide_out[shift - 1, k], top_out[shift - 1, k] = coded(
            *added(bound.at[shift - 1, k], take.at[shift, 0, k]))
        y_copies[shift, k] = y_copy(shift, k)
        for copy in y_copies[shift, k]:
            copy.start()
    for k in range(chunks):
        hand_over(0, k)
    for k in range(chunks):
        put(kept.at[k], partial(core, chip, k))
    for k in range(chunks):
        gives[0, k].wait_recv()
        put(kept.at[k], added(kept.at[k], take.at[0, 0, k]))

    res_copies, near_copies = {}, {}
    for k in range(chunks):
        total = kept[k, 0], kept[k, 1]
        for shift in range(1, chips):
            for copy in y_copies[shift, k]:
                copy.wait_recv()
            total = added(total, decoded(wide_in[shift - 1, k], top_in[shift - 1, k]))
        out[:, columns(core, chip, k)] = (total[0] / total[1]).astype(out.dtype)
        for shift in range(1, chips):
            res_copies[shift, k] = res_copy(shift, k)
            res_copies[shift, k].start()
        near_copies[0, k] = near_copy(0, k)
        near_copies[0, k].start()
    for shift, k in away:
        res_copies[shift, k].wait_recv()
        near_copies[shift, k] = near_copy(shift, k)
        near_copies[shift, k].start()
    for copies in (gives, res_copies):
        for copy in copies.values():
            copy.wait_send()
    for pair in y_copies.values():
        for copy in pair:
            copy.wait_send()
    for copy in stat_copies:
        copy.wait_send()
    for copy in near_copies.values():
        copy.wait()


def local(mesh, params, fisher):
    count, rows, width = fisher.shape
    tasks, groups = mesh.shape["task"], mesh.shape["param"]
    chips, piece = tasks // 2, width // tasks
    chunks = max(1, min(PIECES, piece // LANES))
    chunk = piece // chunks
    far = max(1, chips - 1)
    f32, dma = jnp.float32, pltpu.SemaphoreType.DMA
    return pl.pallas_call(
        functools.partial(kernel, tasks, groups),
        out_shape=pltpu.VMEM((rows, width), jnp.bfloat16),
        in_specs=[pl.BlockSpec(memory_space=pltpu.HBM)] * 2,
        out_specs=pl.BlockSpec(memory_space=pltpu.VMEM),
        scratch_shapes=[
            pltpu.VMEM((count, rows, width), f32),
            pltpu.VMEM((count, rows, width), jnp.bfloat16),
            pltpu.VMEM((groups, 2 * count, LANES), f32),
            pltpu.VMEM((chips, 1, chunks, 2, rows, chunk), f32),
            pltpu.VMEM((chips, 1, chunks, 2, rows, chunk), f32),
            pltpu.VMEM((far, chunks, 2, rows, chunk), f32),
            pltpu.VMEM((chunks, 2, rows, chunk), f32),
            pltpu.VMEM((far, chunks, rows, chunk), f32),
            pltpu.VMEM((far, chunks, rows, chunk), jnp.bfloat16),
            pltpu.VMEM((far, chunks, rows, chunk), f32),
            pltpu.VMEM((far, chunks, rows, chunk), jnp.bfloat16),
            dma((count,)),
            dma((count,)),
            dma((groups,)),
            dma((groups,)),
            dma((chips, chunks)),
            dma((chips, chunks)),
            dma((far, chunks)),
            dma((far, chunks)),
            dma((far, chunks)),
            dma((far, chunks)),
            dma((far, chunks)),
            dma((far, chunks)),
            dma((chips, chunks)),
            dma((chips, chunks)),
        ],
        compiler_params=pltpu.CompilerParams(collective_id=0, has_side_effects=True),
        name="merge",
    )(params, fisher)


def solution(mesh):
    in_specs = (P("task", "param", None), P("task", "param", None))
    out_specs = P("param", None)
    return jax.shard_map(
        functools.partial(local, mesh), mesh=mesh, in_specs=in_specs, out_specs=out_specs, check_vma=False)
```

```python
import functools

import jax
import jax.numpy as jnp
from jax import lax
from jax.experimental import pallas as pl
from jax.experimental.pallas import tpu as pltpu
from jax.sharding import PartitionSpec as P

MESH = pl.DeviceIdType.MESH
LANES = 128
PIECES = 8


def split(value):
    scaled = value * 257.0
    kept = scaled - (scaled - value)
    low = kept * 0.74
    scaled = low * 8388609.0
    return kept, scaled - (scaled - low)


def coded(numer, denom):
    top = numer.astype(jnp.bfloat16)
    wide = top.astype(jnp.float32)
    rest = (numer - wide) / jnp.where(wide == 0.0, 1.0, wide)
    rest = jnp.clip(jnp.round(rest * 32768.0), -127.0, 127.0)
    kept, power = split(denom)
    return kept + rest * (power * (1.0 / 8388608.0)), top


def decoded(carrier, top):
    kept, power = split(carrier)
    wide = top.astype(jnp.float32)
    return wide + wide * ((carrier - kept) / power * 256.0), kept


def kernel(tasks, groups, params_hbm, fisher_hbm, out, fisher, params, stats, give, take, kept,
           wide_out, top_out, wide_in, top_in,
           load_f, load_p, stat_send, stat_recv, give_send, give_recv, y_send, y_recv, top_send, top_recv,
           res_send, res_recv, cross_send, cross_recv, near_send, near_recv):
    count, rows, width = fisher.shape
    chips = tasks // 2
    chunks, chunk = give.shape[2], give.shape[5]
    half, piece = width // 2, width // tasks
    task, param = lax.axis_index("task"), lax.axis_index("param")
    chip, core = task // 2, task % 2
    partner = {"task": chip * 2 + 1 - core, "param": param}

    def chip_at(shift):
        return lax.rem(chip + shift, chips)

    def same_core(shift):
        return {"task": chip_at(shift) * 2 + core, "param": param}

    def member(shift):
        return {"task": task, "param": lax.rem(param + shift, groups)}

    loads_f = [pltpu.make_async_copy(fisher_hbm.at[t], fisher.at[t], load_f.at[t]) for t in range(count)]
    loads_p = [pltpu.make_async_copy(params_hbm.at[t], params.at[t], load_p.at[t]) for t in range(count)]
    for copy in loads_f:
        copy.start()

    barrier = pltpu.get_barrier_semaphore()
    greeted = [member(s) for s in range(1, groups)] + [partner]
    for s in range(1, chips):
        greeted += [same_core(s), {"task": chip_at(s) * 2 + 1 - core, "param": param}]
    for device in greeted:
        pl.semaphore_signal(barrier, inc=1, device_id=device, device_id_type=MESH)

    tops, sums = [], []
    for t in range(count):
        loads_f[t].wait()
        if t == count - 1:
            for copy in loads_p:
                copy.start()

        def over(step, carry, t=t):
            block = fisher[t, :, pl.ds(pl.multiple_of(step * LANES, LANES), LANES)]
            return jnp.maximum(carry[0], block), carry[1] + block

        first = fisher[t, :, 0:LANES]
        top, total = lax.fori_loop(1, width // LANES, over, (first, first), unroll=8)
        tops.append(jnp.max(top, axis=0, keepdims=True))
        sums.append(jnp.sum(total, axis=0, keepdims=True))
    top = jnp.max(jnp.concatenate(tops, axis=0), axis=1, keepdims=True)
    total = jnp.sum(jnp.concatenate(sums, axis=0), axis=1, keepdims=True)
    both = jnp.broadcast_to(jnp.concatenate([top, total], axis=0), (2 * count, LANES))
    lane = lax.broadcasted_iota(jnp.int32, both.shape, 1)
    own_lane = lane == lax.broadcasted_iota(jnp.int32, both.shape, 0)
    stats[0] = jnp.sum(jnp.where(own_lane, both, 0.0), axis=0, keepdims=True)

    pl.semaphore_wait(barrier, len(greeted))

    stat_copies = [
        pltpu.make_async_remote_copy(
            src_ref=stats.at[0], dst_ref=stats.at[s], send_sem=stat_send.at[s], recv_sem=stat_recv.at[s],
            device_id=member(s), device_id_type=MESH)
        for s in range(1, groups)
    ]
    for copy in stat_copies:
        copy.start()
    for copy in loads_p:
        copy.wait()
    for copy in stat_copies:
        copy.wait_recv()
    peak = total = stats[0]
    for s in range(1, groups):
        peak = jnp.maximum(peak, stats[s])
        total = total + stats[s]
    size = float(rows * groups * width)
    spread = []
    for t in range(count):
        gain = size / jnp.broadcast_to(total[:, count + t:count + t + 1], (1, LANES))
        factor = jnp.broadcast_to(peak[:, t:t + 1], (1, LANES)) * gain
        spread.append([jnp.broadcast_to(a, (rows, LANES)) for a in (gain, 0.002 * factor, 0.25 * factor)])

    def partial(side, target, k):
        numers, denoms = [], []
        for part in range(chunk // LANES):
            start = pl.multiple_of(side * half + target * piece + k * chunk + part * LANES, LANES)
            numer = denom = None
            for t in range(count):
                gain_t, low_t, high_t = spread[t]
                info = fisher[t, :, pl.ds(start, LANES)]
                theta = params[t, :, pl.ds(start, LANES)].astype(jnp.float32)
                weight = jnp.minimum(jnp.maximum(info * gain_t, low_t), high_t)
                numer = weight * theta if t == 0 else numer + weight * theta
                denom = weight if t == 0 else denom + weight
            numers.append(numer)
            denoms.append(denom)
        if len(numers) == 1:
            return numers[0], denoms[0]
        return jnp.concatenate(numers, axis=1), jnp.concatenate(denoms, axis=1)

    def put(ref, pair):
        ref[0], ref[1] = pair

    def added(one, two):
        return one[0] + two[0], one[1] + two[1]

    def give_copy(shift, k):
        return pltpu.make_async_remote_copy(
            src_ref=give.at[shift, 0, k], dst_ref=take.at[shift, 0, k], send_sem=give_send.at[shift, k],
            recv_sem=give_recv.at[shift, k], device_id=partner, device_id_type=MESH)

    def y_copy(shift, k):
        return [
            pltpu.make_async_remote_copy(
                src_ref=source.at[shift - 1, k], dst_ref=sink.at[shift - 1, k], send_sem=send.at[shift - 1, k],
                recv_sem=recv.at[shift - 1, k], device_id=same_core(shift), device_id_type=MESH)
            for source, sink, send, recv in (
                (wide_out, wide_in, y_send, y_recv), (top_out, top_in, top_send, top_recv))
        ]

    def columns(side, target, k):
        return pl.ds(pl.multiple_of(side * half + target * piece + k * chunk, LANES), chunk)

    def res_copy(shift, k):
        where = out.at[:, columns(core, chip, k)]
        return pltpu.make_async_remote_copy(
            src_ref=where, dst_ref=where, send_sem=res_send.at[shift - 1, k], recv_sem=res_recv.at[shift - 1, k],
            device_id=same_core(shift), device_id_type=MESH)

    def cross_copy(shift):
        where = out.at[:, columns(core, chip, chunks - 1)]
        return pltpu.make_async_remote_copy(
            src_ref=where, dst_ref=where, send_sem=cross_send.at[shift - 1], recv_sem=cross_recv.at[shift - 1],
            device_id={"task": chip_at(shift) * 2 + 1 - core, "param": param}, device_id_type=MESH)

    def near_copy(shift, k):
        where = out.at[:, columns(core, chip_at(chips - shift), k)]
        return pltpu.make_async_remote_copy(
            src_ref=where, dst_ref=where, send_sem=near_send.at[shift, k], recv_sem=near_recv.at[shift, k],
            device_id=partner, device_id_type=MESH)

    away = [(shift, k) for k in range(chunks) for shift in range(1, chips)]
    gives = {}

    def hand_over(shift, k):
        put(give.at[shift, 0, k], partial(1 - core, chip_at(shift), k))
        gives[shift, k] = give_copy(shift, k)
        gives[shift, k].start()

    for shift, k in away:
        hand_over(shift, k)
    y_copies = {}
    for shift, k in away:
        own = partial(core, chip_at(shift), k)
        gives[shift, k].wait_recv()
        wide_out[shift - 1, k], top_out[shift - 1, k] = coded(*added(own, take.at[shift, 0, k]))
        y_copies[shift, k] = y_copy(shift, k)
        for copy in y_copies[shift, k]:
            copy.start()
    for k in range(chunks):
        hand_over(0, k)
    for k in range(chunks):
        own = partial(core, chip, k)
        gives[0, k].wait_recv()
        put(kept.at[k], added(own, take.at[0, 0, k]))

    res_copies, near_copies = {}, {}
    for k in range(chunks):
        total = kept[k, 0], kept[k, 1]
        for shift in range(1, chips):
            for copy in y_copies[shift, k]:
                copy.wait_recv()
            total = added(total, decoded(wide_in[shift - 1, k], top_in[shift - 1, k]))
        out[:, columns(core, chip, k)] = (total[0] / total[1]).astype(out.dtype)
        for shift in range(1, chips):
            res_copies[shift, k] = res_copy(shift, k)
            res_copies[shift, k].start()
        near_copies[0, k] = near_copy(0, k)
        near_copies[0, k].start()
    crosses = [cross_copy(shift) for shift in range(1, chips)]
    for copy in crosses:
        copy.start()
    for shift, k in away:
        res_copies[shift, k].wait_recv()
        if k < chunks - 1:
            near_copies[shift, k] = near_copy(shift, k)
            near_copies[shift, k].start()
    for copy in crosses:
        copy.wait()
    for copies in (gives, res_copies):
        for copy in copies.values():
            copy.wait_send()
    for pair in y_copies.values():
        for copy in pair:
            copy.wait_send()
    for copy in stat_copies:
        copy.wait_send()
    for copy in near_copies.values():
        copy.wait()


def local(mesh, params, fisher):
    count, rows, width = fisher.shape
    tasks, groups = mesh.shape["task"], mesh.shape["param"]
    chips, piece = tasks // 2, width // tasks
    chunks = max(1, min(PIECES, piece // LANES))
    chunk = piece // chunks
    far = max(1, chips - 1)
    f32, dma = jnp.float32, pltpu.SemaphoreType.DMA
    return pl.pallas_call(
        functools.partial(kernel, tasks, groups),
        out_shape=pltpu.VMEM((rows, width), jnp.bfloat16),
        in_specs=[pl.BlockSpec(memory_space=pltpu.HBM)] * 2,
        out_specs=pl.BlockSpec(memory_space=pltpu.VMEM),
        scratch_shapes=[
            pltpu.VMEM((count, rows, width), f32),
            pltpu.VMEM((count, rows, width), jnp.bfloat16),
            pltpu.VMEM((groups, 1, LANES), f32),
            pltpu.VMEM((chips, 1, chunks, 2, rows, chunk), f32),
            pltpu.VMEM((chips, 1, chunks, 2, rows, chunk), f32),
            pltpu.VMEM((chunks, 2, rows, chunk), f32),
            pltpu.VMEM((far, chunks, rows, chunk), f32),
            pltpu.VMEM((far, chunks, rows, chunk), jnp.bfloat16),
            pltpu.VMEM((far, chunks, rows, chunk), f32),
            pltpu.VMEM((far, chunks, rows, chunk), jnp.bfloat16),
            dma((count,)),
            dma((count,)),
            dma((groups,)),
            dma((groups,)),
            dma((chips, chunks)),
            dma((chips, chunks)),
            dma((far, chunks)),
            dma((far, chunks)),
            dma((far, chunks)),
            dma((far, chunks)),
            dma((far, chunks)),
            dma((far, chunks)),
            dma((far,)),
            dma((far,)),
            dma((chips, chunks)),
            dma((chips, chunks)),
        ],
        compiler_params=pltpu.CompilerParams(collective_id=0, has_side_effects=True),
        name="merge",
    )(params, fisher)


def solution(mesh):
    in_specs = (P("task", "param", None), P("task", "param", None))
    out_specs = P("param", None)
    return jax.shard_map(
        functools.partial(local, mesh), mesh=mesh, in_specs=in_specs, out_specs=out_specs, check_vma=False)
```

```python
import functools

import jax
import jax.numpy as jnp
from jax import lax
from jax.experimental import pallas as pl
from jax.experimental.pallas import tpu as pltpu
from jax.sharding import PartitionSpec as P

MESH = pl.DeviceIdType.MESH
LANES = 128
PIECES = 8


def split(value):
    scaled = value * 257.0
    kept = scaled - (scaled - value)
    low = kept * 0.74
    scaled = low * 8388609.0
    return kept, scaled - (scaled - low)


def coded(numer, denom):
    top = numer.astype(jnp.bfloat16)
    wide = top.astype(jnp.float32)
    rest = (numer - wide) / jnp.where(wide == 0.0, 1.0, wide)
    rest = jnp.clip(jnp.round(rest * 32768.0), -127.0, 127.0)
    kept, power = split(denom)
    return kept + rest * (power * (1.0 / 8388608.0)), top


def decoded(carrier, top):
    kept, power = split(carrier)
    wide = top.astype(jnp.float32)
    return wide + wide * ((carrier - kept) / power * 256.0), kept


def kernel(tasks, groups, params_hbm, fisher_hbm, out, fisher, params, stats, give, take, kept,
           wide_out, top_out, wide_in, top_in,
           load_f, load_p, stat_send, stat_recv, give_send, give_recv, kept_recv, y_send, y_recv, top_send, top_recv,
           res_send, res_recv, cross_send, cross_recv, near_send, near_recv):
    count, rows, width = fisher.shape
    chips = tasks // 2
    chunks, chunk = give.shape[2], give.shape[5]
    half, piece = width // 2, width // tasks
    task, param = lax.axis_index("task"), lax.axis_index("param")
    chip, core = task // 2, task % 2
    partner = {"task": chip * 2 + 1 - core, "param": param}

    def chip_at(shift):
        return lax.rem(chip + shift, chips)

    def same_core(shift):
        return {"task": chip_at(shift) * 2 + core, "param": param}

    def member(shift):
        return {"task": task, "param": lax.rem(param + shift, groups)}

    def drain(ref, semaphore):
        pltpu.make_async_copy(ref, ref, semaphore).wait()

    loads_f = [pltpu.make_async_copy(fisher_hbm.at[t], fisher.at[t], load_f.at[t]) for t in range(count)]
    loads_p = [pltpu.make_async_copy(params_hbm.at[t], params.at[t], load_p) for t in range(count)]
    for copy in loads_f:
        copy.start()

    barrier = pltpu.get_barrier_semaphore()
    greeted = [member(s) for s in range(1, groups)] + [partner]
    for s in range(1, chips):
        greeted += [same_core(s), {"task": chip_at(s) * 2 + 1 - core, "param": param}]
    for device in greeted:
        pl.semaphore_signal(barrier, inc=1, device_id=device, device_id_type=MESH)

    tops, sums = [], []
    for t in range(count):
        loads_f[t].wait()
        if t == count - 1:
            for copy in loads_p:
                copy.start()

        def over(step, carry, t=t):
            block = fisher[t, :, pl.ds(pl.multiple_of(step * LANES, LANES), LANES)]
            return jnp.maximum(carry[0], block), carry[1] + block

        first = fisher[t, :, 0:LANES]
        top, total = lax.fori_loop(1, width // LANES, over, (first, first), unroll=8)
        tops.append(jnp.max(top, axis=0, keepdims=True))
        sums.append(jnp.sum(total, axis=0, keepdims=True))
    top = jnp.max(jnp.concatenate(tops, axis=0), axis=1, keepdims=True)
    total = jnp.sum(jnp.concatenate(sums, axis=0), axis=1, keepdims=True)
    both = jnp.broadcast_to(jnp.concatenate([top, total], axis=0), (2 * count, LANES))
    lane = lax.broadcasted_iota(jnp.int32, both.shape, 1)
    own_lane = lane == lax.broadcasted_iota(jnp.int32, both.shape, 0)
    stats[0] = jnp.sum(jnp.where(own_lane, both, 0.0), axis=0, keepdims=True)

    pl.semaphore_wait(barrier, len(greeted))

    stat_copies = [
        pltpu.make_async_remote_copy(
            src_ref=stats.at[0], dst_ref=stats.at[s], send_sem=stat_send, recv_sem=stat_recv,
            device_id=member(s), device_id_type=MESH)
        for s in range(1, groups)
    ]
    for copy in stat_copies:
        copy.start()
    drain(params, load_p)
    drain(stats.at[1:groups], stat_recv)
    peak = total = stats[0]
    for s in range(1, groups):
        peak = jnp.maximum(peak, stats[s])
        total = total + stats[s]
    size = float(rows * groups * width)
    spread = []
    for t in range(count):
        gain = size / jnp.broadcast_to(total[:, count + t:count + t + 1], (1, LANES))
        factor = jnp.broadcast_to(peak[:, t:t + 1], (1, LANES)) * gain
        spread.append([jnp.broadcast_to(a, (rows, LANES)) for a in (gain, 0.002 * factor, 0.25 * factor)])

    def partial(side, target, k):
        numers, denoms = [], []
        for part in range(chunk // LANES):
            start = pl.multiple_of(side * half + target * piece + k * chunk + part * LANES, LANES)
            numer = denom = None
            for t in range(count):
                gain_t, low_t, high_t = spread[t]
                info = fisher[t, :, pl.ds(start, LANES)]
                theta = params[t, :, pl.ds(start, LANES)].astype(jnp.float32)
                weight = jnp.minimum(jnp.maximum(info * gain_t, low_t), high_t)
                numer = weight * theta if t == 0 else numer + weight * theta
                denom = weight if t == 0 else denom + weight
            numers.append(numer)
            denoms.append(denom)
        if len(numers) == 1:
            return numers[0], denoms[0]
        return jnp.concatenate(numers, axis=1), jnp.concatenate(denoms, axis=1)

    def put(ref, pair):
        ref[0], ref[1] = pair

    def added(one, two):
        return one[0] + two[0], one[1] + two[1]

    def give_copy(shift, k):
        return pltpu.make_async_remote_copy(
            src_ref=give.at[shift, 0, k], dst_ref=take.at[shift, 0, k], send_sem=give_send,
            recv_sem=give_recv.at[shift - 1, k] if shift else kept_recv, device_id=partner, device_id_type=MESH)

    def y_copy(shift, k):
        return [
            pltpu.make_async_remote_copy(
                src_ref=source.at[shift - 1, k], dst_ref=sink.at[shift - 1, k], send_sem=send,
                recv_sem=recv.at[shift - 1, k], device_id=same_core(shift), device_id_type=MESH)
            for source, sink, send, recv in (
                (wide_out, wide_in, y_send, y_recv), (top_out, top_in, top_send, top_recv))
        ]

    def columns(side, target, k):
        return pl.ds(pl.multiple_of(side * half + target * piece + k * chunk, LANES), chunk)

    def res_copy(shift, k):
        where = out.at[:, columns(core, chip, k)]
        return pltpu.make_async_remote_copy(
            src_ref=where, dst_ref=where, send_sem=res_send.at[shift - 1], recv_sem=res_recv.at[shift - 1, k],
            device_id=same_core(shift), device_id_type=MESH)

    def cross_copy(shift):
        where = out.at[:, columns(core, chip, chunks - 1)]
        return pltpu.make_async_remote_copy(
            src_ref=where, dst_ref=where, send_sem=cross_send.at[shift - 1], recv_sem=cross_recv.at[shift - 1],
            device_id={"task": chip_at(shift) * 2 + 1 - core, "param": param}, device_id_type=MESH)

    def near_copy(shift, k):
        where = out.at[:, columns(core, chip_at(chips - shift), k)]
        return pltpu.make_async_remote_copy(
            src_ref=where, dst_ref=where, send_sem=near_send.at[shift], recv_sem=near_recv.at[shift],
            device_id=partner, device_id_type=MESH)

    away = [(shift, k) for k in range(chunks) for shift in range(1, chips)]
    gives = {}

    def hand_over(shift, k):
        put(give.at[shift, 0, k], partial(1 - core, chip_at(shift), k))
        gives[shift, k] = give_copy(shift, k)
        gives[shift, k].start()

    for shift, k in away:
        hand_over(shift, k)
    y_copies = {}
    for shift, k in away:
        own = partial(core, chip_at(shift), k)
        gives[shift, k].wait_recv()
        wide_out[shift - 1, k], top_out[shift - 1, k] = coded(*added(own, take.at[shift, 0, k]))
        y_copies[shift, k] = y_copy(shift, k)
        for copy in y_copies[shift, k]:
            copy.start()
    for k in range(chunks):
        hand_over(0, k)
    for k in range(chunks):
        put(kept.at[k], partial(core, chip, k))
    drain(take.at[0], kept_recv)

    res_copies, near_copies = {}, {}
    for k in range(chunks):
        total = added(kept.at[k], take.at[0, 0, k])
        for shift in range(1, chips):
            for copy in y_copies[shift, k]:
                copy.wait_recv()
            total = added(total, decoded(wide_in[shift - 1, k], top_in[shift - 1, k]))
        out[:, columns(core, chip, k)] = (total[0] / total[1]).astype(out.dtype)
        for shift in range(1, chips):
            res_copies[shift, k] = res_copy(shift, k)
            res_copies[shift, k].start()
        near_copies[0, k] = near_copy(0, k)
        near_copies[0, k].start()
    crosses = [cross_copy(shift) for shift in range(1, chips)]
    for copy in crosses:
        copy.start()
    for shift, k in away:
        res_copies[shift, k].wait_recv()
        if k < chunks - 1:
            near_copies[shift, k] = near_copy(shift, k)
            near_copies[shift, k].start()
    for copy in crosses:
        copy.wait()
    drain(stats.at[1:groups], stat_send)
    drain(give, give_send)
    drain(wide_out, y_send)
    drain(top_out, top_send)
    for shift in range(chips):
        passed = out.at[:, 0:piece - chunk if shift else piece]
        if shift:
            drain(out.at[:, 0:piece], res_send.at[shift - 1])
        if chunks > 1 or not shift:
            drain(passed, near_send.at[shift])
            drain(passed, near_recv.at[shift])


def local(mesh, params, fisher):
    count, rows, width = fisher.shape
    tasks, groups = mesh.shape["task"], mesh.shape["param"]
    chips, piece = tasks // 2, width // tasks
    chunks = max(1, min(PIECES, piece // LANES))
    chunk = piece // chunks
    far = max(1, chips - 1)
    f32, dma = jnp.float32, pltpu.SemaphoreType.DMA
    return pl.pallas_call(
        functools.partial(kernel, tasks, groups),
        out_shape=pltpu.VMEM((rows, width), jnp.bfloat16),
        in_specs=[pl.BlockSpec(memory_space=pltpu.HBM)] * 2,
        out_specs=pl.BlockSpec(memory_space=pltpu.VMEM),
        scratch_shapes=[
            pltpu.VMEM((count, rows, width), f32),
            pltpu.VMEM((count, rows, width), jnp.bfloat16),
            pltpu.VMEM((groups, 1, LANES), f32),
            pltpu.VMEM((chips, 1, chunks, 2, rows, chunk), f32),
            pltpu.VMEM((chips, 1, chunks, 2, rows, chunk), f32),
            pltpu.VMEM((chunks, 2, rows, chunk), f32),
            pltpu.VMEM((far, chunks, rows, chunk), f32),
            pltpu.VMEM((far, chunks, rows, chunk), jnp.bfloat16),
            pltpu.VMEM((far, chunks, rows, chunk), f32),
            pltpu.VMEM((far, chunks, rows, chunk), jnp.bfloat16),
            dma((count,)),
            dma,
            dma,
            dma,
            dma,
            dma((far, chunks)),
            dma,
            dma,
            dma((far, chunks)),
            dma,
            dma((far, chunks)),
            dma((far,)),
            dma((far, chunks)),
            dma((far,)),
            dma((far,)),
            dma((chips,)),
            dma((chips,)),
        ],
        compiler_params=pltpu.CompilerParams(collective_id=0, has_side_effects=True),
        name="merge",
    )(params, fisher)


def solution(mesh):
    in_specs = (P("task", "param", None), P("task", "param", None))
    out_specs = P("param", None)
    return jax.shard_map(
        functools.partial(local, mesh), mesh=mesh, in_specs=in_specs, out_specs=out_specs, check_vma=False)
```

```python
import functools

import jax
import jax.numpy as jnp
from jax import lax
from jax.experimental import pallas as pl
from jax.experimental.pallas import tpu as pltpu
from jax.sharding import PartitionSpec as P

MESH = pl.DeviceIdType.MESH
LANES = 128
PIECES = 8
AHEAD = 3


def split(value):
    scaled = value * 257.0
    kept = scaled - (scaled - value)
    low = kept * 0.74
    scaled = low * 8388609.0
    return kept, scaled - (scaled - low)


def coded(numer, denom):
    top = numer.astype(jnp.bfloat16)
    wide = top.astype(jnp.float32)
    rest = (numer - wide) / jnp.where(wide == 0.0, 1.0, wide)
    rest = jnp.clip(jnp.round(rest * 32768.0), -127.0, 127.0)
    kept, power = split(denom)
    return kept + rest * (power * (1.0 / 8388608.0)), top


def decoded(carrier, top):
    kept, power = split(carrier)
    wide = top.astype(jnp.float32)
    return wide + wide * ((carrier - kept) / power * 256.0), kept


def kernel(tasks, groups, params_hbm, fisher_hbm, out, fisher, params, stats, give, take, kept,
           wide_out, top_out, wide_in, top_in,
           load_f, load_p, stat_send, stat_recv, give_send, give_recv, kept_recv, y_send, y_recv, top_send, top_recv,
           res_send, res_recv, cross_send, cross_recv, near_send, near_recv):
    count, rows, width = fisher.shape
    chips = tasks // 2
    chunks, chunk = give.shape[2], give.shape[5]
    half, piece = width // 2, width // tasks
    task, param = lax.axis_index("task"), lax.axis_index("param")
    chip, core = task // 2, task % 2
    partner = {"task": chip * 2 + 1 - core, "param": param}

    def chip_at(shift):
        return lax.rem(chip + shift, chips)

    def same_core(shift):
        return {"task": chip_at(shift) * 2 + core, "param": param}

    def member(shift):
        return {"task": task, "param": lax.rem(param + shift, groups)}

    def drain(ref, semaphore):
        pltpu.make_async_copy(ref, ref, semaphore).wait()

    spans = [(t, 0, width) for t in range(count - 1)] + [(count - 1, 0, half), (count - 1, half, half)]
    loads_f = [
        pltpu.make_async_copy(
            fisher_hbm.at[t, :, pl.ds(start, size)], fisher.at[t, :, pl.ds(start, size)], load_f.at[n])
        for n, (t, start, size) in enumerate(spans)
    ]
    loads_p = [pltpu.make_async_copy(params_hbm.at[t], params.at[t], load_p) for t in range(count)]
    for copy in loads_f:
        copy.start()

    barrier = pltpu.get_barrier_semaphore()
    greeted = [member(s) for s in range(1, groups)] + [partner]
    for s in range(1, chips):
        greeted += [same_core(s), {"task": chip_at(s) * 2 + 1 - core, "param": param}]
    for device in greeted:
        pl.semaphore_signal(barrier, inc=1, device_id=device, device_id_type=MESH)

    tops, sums = [], []
    for n, (t, start, size) in enumerate(spans):
        loads_f[n].wait()
        if n == count:
            for copy in loads_p:
                copy.start()

        def over(step, carry, t=t):
            block = fisher[t, :, pl.ds(pl.multiple_of(step * LANES, LANES), LANES)]
            return jnp.maximum(carry[0], block), carry[1] + block

        begin = start // LANES
        if start == 0:
            first = fisher[t, :, 0:LANES]
            top, total, begin = first, first, 1
        top, total = lax.fori_loop(begin, (start + size) // LANES, over, (top, total), unroll=8)
        if start + size == width:
            tops.append(jnp.max(top, axis=0, keepdims=True))
            sums.append(jnp.sum(total, axis=0, keepdims=True))
    top = jnp.max(jnp.concatenate(tops, axis=0), axis=1, keepdims=True)
    total = jnp.sum(jnp.concatenate(sums, axis=0), axis=1, keepdims=True)
    both = jnp.broadcast_to(jnp.concatenate([top, total], axis=0), (2 * count, LANES))
    lane = lax.broadcasted_iota(jnp.int32, both.shape, 1)
    own_lane = lane == lax.broadcasted_iota(jnp.int32, both.shape, 0)
    stats[0] = jnp.sum(jnp.where(own_lane, both, 0.0), axis=0, keepdims=True)

    pl.semaphore_wait(barrier, len(greeted))

    stat_copies = [
        pltpu.make_async_remote_copy(
            src_ref=stats.at[0], dst_ref=stats.at[s], send_sem=stat_send, recv_sem=stat_recv,
            device_id=member(s), device_id_type=MESH)
        for s in range(1, groups)
    ]
    for copy in stat_copies:
        copy.start()
    drain(params, load_p)
    drain(stats.at[1:groups], stat_recv)
    peak = total = stats[0]
    for s in range(1, groups):
        peak = jnp.maximum(peak, stats[s])
        total = total + stats[s]
    size = float(rows * groups * width)
    spread = []
    for t in range(count):
        gain = size / jnp.broadcast_to(total[:, count + t:count + t + 1], (1, LANES))
        factor = jnp.broadcast_to(peak[:, t:t + 1], (1, LANES)) * gain
        spread.append([jnp.broadcast_to(a, (rows, LANES)) for a in (gain, 0.002 * factor, 0.25 * factor)])

    def partial(side, target, k):
        numers, denoms = [], []
        for part in range(chunk // LANES):
            start = pl.multiple_of(side * half + target * piece + k * chunk + part * LANES, LANES)
            numer = denom = None
            for t in range(count):
                gain_t, low_t, high_t = spread[t]
                info = fisher[t, :, pl.ds(start, LANES)]
                theta = params[t, :, pl.ds(start, LANES)].astype(jnp.float32)
                weight = jnp.minimum(jnp.maximum(info * gain_t, low_t), high_t)
                numer = weight * theta if t == 0 else numer + weight * theta
                denom = weight if t == 0 else denom + weight
            numers.append(numer)
            denoms.append(denom)
        if len(numers) == 1:
            return numers[0], denoms[0]
        return jnp.concatenate(numers, axis=1), jnp.concatenate(denoms, axis=1)

    def put(ref, pair):
        ref[0], ref[1] = pair

    def added(one, two):
        return one[0] + two[0], one[1] + two[1]

    def give_copy(shift, k):
        return pltpu.make_async_remote_copy(
            src_ref=give.at[shift, 0, k], dst_ref=take.at[shift, 0, k], send_sem=give_send,
            recv_sem=give_recv.at[shift - 1, k] if shift else kept_recv, device_id=partner, device_id_type=MESH)

    def y_copy(shift, k):
        return [
            pltpu.make_async_remote_copy(
                src_ref=source.at[shift - 1, k], dst_ref=sink.at[shift - 1, k], send_sem=send,
                recv_sem=recv.at[shift - 1, k], device_id=same_core(shift), device_id_type=MESH)
            for source, sink, send, recv in (
                (wide_out, wide_in, y_send, y_recv), (top_out, top_in, top_send, top_recv))
        ]

    def columns(side, target, k):
        return pl.ds(pl.multiple_of(side * half + target * piece + k * chunk, LANES), chunk)

    def res_copy(shift, k):
        where = out.at[:, columns(core, chip, k)]
        return pltpu.make_async_remote_copy(
            src_ref=where, dst_ref=where, send_sem=res_send.at[shift - 1], recv_sem=res_recv.at[shift - 1, k],
            device_id=same_core(shift), device_id_type=MESH)

    def cross_copy(shift):
        where = out.at[:, columns(core, chip, chunks - 1)]
        return pltpu.make_async_remote_copy(
            src_ref=where, dst_ref=where, send_sem=cross_send.at[shift - 1], recv_sem=cross_recv.at[shift - 1],
            device_id={"task": chip_at(shift) * 2 + 1 - core, "param": param}, device_id_type=MESH)

    def near_copy(shift, k):
        where = out.at[:, columns(core, chip_at(chips - shift), k)]
        return pltpu.make_async_remote_copy(
            src_ref=where, dst_ref=where, send_sem=near_send.at[shift], recv_sem=near_recv.at[shift],
            device_id=partner, device_id_type=MESH)

    away = [(shift, k) for k in range(chunks) for shift in range(1, chips)]
    gives = {}

    def hand_over(shift, k):
        put(give.at[shift, 0, k], partial(1 - core, chip_at(shift), k))
        gives[shift, k] = give_copy(shift, k)
        gives[shift, k].start()

    for shift, k in away[:AHEAD]:
        hand_over(shift, k)
    y_copies = {}
    for n, (shift, k) in enumerate(away):
        own = partial(core, chip_at(shift), k)
        gives[shift, k].wait_recv()
        wide_out[shift - 1, k], top_out[shift - 1, k] = coded(*added(own, take.at[shift, 0, k]))
        y_copies[shift, k] = y_copy(shift, k)
        for copy in y_copies[shift, k]:
            copy.start()
        if n + AHEAD < len(away):
            hand_over(*away[n + AHEAD])
    for k in range(chunks):
        hand_over(0, k)
    for k in range(chunks):
        put(kept.at[k], partial(core, chip, k))
    drain(take.at[0], kept_recv)

    res_copies, near_copies = {}, {}
    for k in range(chunks):
        total = added(kept.at[k], take.at[0, 0, k])
        for shift in range(1, chips):
            for copy in y_copies[shift, k]:
                copy.wait_recv()
            total = added(total, decoded(wide_in[shift - 1, k], top_in[shift - 1, k]))
        out[:, columns(core, chip, k)] = (total[0] / total[1]).astype(out.dtype)
        for shift in range(1, chips):
            res_copies[shift, k] = res_copy(shift, k)
            res_copies[shift, k].start()
        near_copies[0, k] = near_copy(0, k)
        near_copies[0, k].start()
    crosses = [cross_copy(shift) for shift in range(1, chips)]
    for copy in crosses:
        copy.start()
    for shift, k in away:
        res_copies[shift, k].wait_recv()
        if k < chunks - 1:
            near_copies[shift, k] = near_copy(shift, k)
            near_copies[shift, k].start()
    for copy in crosses:
        copy.wait()
    drain(stats.at[1:groups], stat_send)
    drain(give, give_send)
    drain(wide_out, y_send)
    drain(top_out, top_send)
    for shift in range(chips):
        passed = out.at[:, 0:piece - chunk if shift else piece]
        if shift:
            drain(out.at[:, 0:piece], res_send.at[shift - 1])
        if chunks > 1 or not shift:
            drain(passed, near_send.at[shift])
            drain(passed, near_recv.at[shift])


def local(mesh, params, fisher):
    count, rows, width = fisher.shape
    tasks, groups = mesh.shape["task"], mesh.shape["param"]
    chips, piece = tasks // 2, width // tasks
    chunks = max(1, min(PIECES, piece // LANES))
    chunk = piece // chunks
    far = max(1, chips - 1)
    f32, dma = jnp.float32, pltpu.SemaphoreType.DMA
    return pl.pallas_call(
        functools.partial(kernel, tasks, groups),
        out_shape=pltpu.VMEM((rows, width), jnp.bfloat16),
        in_specs=[pl.BlockSpec(memory_space=pltpu.HBM)] * 2,
        out_specs=pl.BlockSpec(memory_space=pltpu.VMEM),
        scratch_shapes=[
            pltpu.VMEM((count, rows, width), f32),
            pltpu.VMEM((count, rows, width), jnp.bfloat16),
            pltpu.VMEM((groups, 1, LANES), f32),
            pltpu.VMEM((chips, 1, chunks, 2, rows, chunk), f32),
            pltpu.VMEM((chips, 1, chunks, 2, rows, chunk), f32),
            pltpu.VMEM((chunks, 2, rows, chunk), f32),
            pltpu.VMEM((far, chunks, rows, chunk), f32),
            pltpu.VMEM((far, chunks, rows, chunk), jnp.bfloat16),
            pltpu.VMEM((far, chunks, rows, chunk), f32),
            pltpu.VMEM((far, chunks, rows, chunk), jnp.bfloat16),
            dma((count + 1,)),
            dma,
            dma,
            dma,
            dma,
            dma((far, chunks)),
            dma,
            dma,
            dma((far, chunks)),
            dma,
            dma((far, chunks)),
            dma((far,)),
            dma((far, chunks)),
            dma((far,)),
            dma((far,)),
            dma((chips,)),
            dma((chips,)),
        ],
        compiler_params=pltpu.CompilerParams(collective_id=0, has_side_effects=True),
        name="merge",
    )(params, fisher)


def solution(mesh):
    in_specs = (P("task", "param", None), P("task", "param", None))
    out_specs = P("param", None)
    return jax.shard_map(
        functools.partial(local, mesh), mesh=mesh, in_specs=in_specs, out_specs=out_specs, check_vma=False)
```
